32 devices in a mesh: grp: 2 (over core), mr: 8 (over z, y), mc: 2 (over x).
Axes of the slice: x: 2, y: 2, z: 4, core: 2. Of those that a mesh axis runs over, the one named last changes fastest.
Arguments:
- queries: bfloat16 [384, 8192], P(('grp', 'mr'), 'mc'), may hold values from -6 to 6
- new_keys: bfloat16 [384, 1024], P(('grp', 'mr'), 'mc'), may hold values from -6 to 6
- new_values: bfloat16 [384, 1024], P(('grp', 'mr'), 'mc'), may hold values from -6 to 6
- key_cache: bfloat16 [384, 512, 1024], P(('grp', 'mr'), None, 'mc'), may hold values from -6 to 6
- value_cache: bfloat16 [384, 512, 1024], P(('grp', 'mr'), None, 'mc'), may hold values from -6 to 6
- context_len: int32 [384], P(('grp', 'mr')), may hold values from 2 to 512, as said below
- cache_slot: int32 [384], P(('grp', 'mr')), may hold values from 0 to 383, as said below
- residual_in: bfloat16 [384, 8192], P(('grp', 'mr'), 'mc'), may hold values from -31 to 31
- out_weight: bfloat16 [8192, 8192], P(('grp', 'mr'), 'mc'), may hold values from -0.25 to 0.25
- gate_weight: bfloat16 [8192, 28672], P('mc', ('grp', 'mr')), may hold values from -0.0625 to 0.0625
- up_weight: bfloat16 [8192, 28672], P('mc', ('grp', 'mr')), may hold values from -0.0625 to 0.0625
Outputs:
- residual_out: bfloat16 [384, 8192], P(('grp', 'mr'), 'mc')
- activation: bfloat16 [384, 28672], P('mc', ('grp', 'mr'))
The draws below stay inside these ranges and needn't reach their ends.
Inputs may be any that keep to these rules, and one draw needn't show every extreme that they name: Row r's history fills positions 0 to context_len[r] - 1 of its cache row; some row has 512. `cache_slot`: within each aligned block of 24 rows the values are a permutation of that block's own row indices.
All inputs are finite; a program needn't handle non-finite values.
Results may differ from the reference program's by a relative error of at most 0.006.
Values may be sent and summed in bfloat16 or wider, within the bound.
A program may use at most 128 MiB of HBM per device.

```python
import jax
import jax.numpy as jnp
from jax import lax

D = 8192
H = 64
KVH = 8
HD = 128
FF = 28672
CTX = 512
ROWS_DEV = 24
ROWS = 384


def draw_queries(key, part):
    current_key = jax.random.fold_in(key, 17)
    values = jax.random.truncated_normal(current_key, -6.0, 6.0, (ROWS, H * HD), jnp.float32)
    return values.astype(jnp.bfloat16)


def draw_key_cache(key, part):
    current_key = jax.random.fold_in(key, 29)
    values = jax.random.truncated_normal(current_key, -6.0, 6.0, (ROWS, CTX, KVH * HD), jnp.float32)
    return values.astype(jnp.bfloat16)


def draw_residual_in(key, part):
    column = jnp.arange(D, dtype=jnp.float32) / D
    values = jax.random.truncated_normal(key, -6.0, 6.0, (ROWS, D), jnp.float32) * (3.0 ** column)[None, :]
    return values.astype(jnp.bfloat16)


def draw_context_len(key, part):
    length_key, longest_key = jax.random.split(jax.random.fold_in(key, 41))
    values = jax.random.randint(length_key, (ROWS,), 2, CTX + 1)
    longest = jax.random.randint(longest_key, (), 0, ROWS)
    return jnp.where(jnp.arange(ROWS) == longest, CTX, values).astype(jnp.int32)


def shuffle_block(tile_key_rows):
    return jax.random.permutation(tile_key_rows, ROWS_DEV)


def draw_cache_slot(key, part):
    block_count = ROWS // ROWS_DEV
    block_keys = jax.random.split(jax.random.fold_in(key, 53), block_count)
    orders = jax.vmap(shuffle_block)(block_keys)
    offsets = jnp.arange(block_count, dtype=jnp.int32)[:, None] * ROWS_DEV
    return (orders.astype(jnp.int32) + offsets).reshape(ROWS).astype(jnp.int32)


def block_scale(key, dims, cuts, low, largest):
    gain = 1.0
    for dim, blocks in cuts:
        draws = jax.random.uniform(jax.random.fold_in(jax.random.fold_in(key, 6), dim), (blocks,), jnp.float32, low / len(cuts), largest / len(cuts))
        gain = gain * jnp.repeat(jnp.exp(draws), dims[dim] // blocks).reshape((-1,) + (1,) * (len(dims) - 1 - dim))
    return gain


def scatter_about(rng, shape, scale, bound, pieces=(), kind=jnp.bfloat16):
    array = jax.random.normal(rng, shape, jnp.float32) * scale
    if len(pieces) > 0:
        array = block_scale(rng, shape, pieces, -0.22, 0.18) * array
    return jnp.clip(array, min=-bound, max=bound).astype(kind)


def setup_inputs(seed: int = 0) -> dict:
    key_list = jax.random.split(jax.random.key(seed), 12)
    queries = draw_queries(jax.random.fold_in(key_list[11], 71), 0)
    new_keys = scatter_about(key_list[1], (ROWS, KVH * HD), 1.0, 6.0, ((0, 16), (1, 2)))
    new_values = scatter_about(key_list[2], (ROWS, KVH * HD), 1.0, 6.0, ((0, 16), (1, 2)))
    key_cache = draw_key_cache(jax.random.fold_in(key_list[11], 71), 0)
    value_cache = scatter_about(key_list[4], (ROWS, CTX, KVH * HD), 1.0, 6.0, ((0, 16), (2, 2)))
    context_len = draw_context_len(jax.random.fold_in(key_list[11], 71), 0)
    cache_slot = draw_cache_slot(jax.random.fold_in(key_list[11], 71), 0)
    residual_in = draw_residual_in(jax.random.fold_in(key_list[11], 71), 0)
    out_weight = scatter_about(key_list[8], (H * HD, D), (H * 8) ** -0.5, 0.25, ((0, 16), (1, 2)))
    gate_weight = scatter_about(key_list[9], (D, FF), D ** -0.5, 0.0625, ((0, 2), (1, 16)))
    up_weight = scatter_about(key_list[10], (D, FF), D ** -0.5, 0.0625, ((0, 2), (1, 16)))
    return {"queries": queries, "new_keys": new_keys, "new_values": new_values, "key_cache": key_cache, "value_cache": value_cache, "context_len": context_len, "cache_slot": cache_slot, "residual_in": residual_in, "out_weight": out_weight, "gate_weight": gate_weight, "up_weight": up_weight}


norm_epsilon = 1e-05
masked_score = -1e+30

def attend_block(queries, new_keys, new_values, key_rows, value_rows, context_len):
    row_denominator_sum = queries.shape[0]
    kv_heads = key_rows.shape[2] // HD
    groups = queries.shape[1] // key_rows.shape[2]
    attention_logit_scale = HD ** (-0.5)
    query_grouped_four = queries.astype(jnp.float32).reshape(row_denominator_sum, kv_heads, groups, HD)
    key_four = key_rows.astype(jnp.float32).reshape(row_denominator_sum, CTX, kv_heads, HD)
    value_four = value_rows.astype(jnp.float32).reshape(row_denominator_sum, CTX, kv_heads, HD)
    current_key = new_keys.astype(jnp.float32).reshape(row_denominator_sum, kv_heads, HD)
    own_value = new_values.astype(jnp.float32).reshape(row_denominator_sum, kv_heads, HD)
    scores = jnp.einsum('bkgd,bckd->bkgc', query_grouped_four, key_four) * attention_logit_scale
    positions = jnp.arange(CTX, dtype=jnp.int32)
    valid_mask = positions[None, :] < context_len[:, None]
    scores = jnp.where(valid_mask[:, None, None, :], scores, masked_score)
    current_score = jnp.einsum('cnhz,cnz->cnh', query_grouped_four, current_key) * attention_logit_scale
    row_max = jnp.maximum(lax.optimization_barrier(jnp.max(scores, axis=3)), current_score)
    exponent = jnp.exp(scores - row_max[..., None])
    own_exponent = jnp.exp(current_score - row_max)
    denominator = lax.optimization_barrier(jnp.sum(exponent, axis=3)) + own_exponent
    weights = lax.optimization_barrier((exponent / denominator[..., None]).astype(jnp.bfloat16)).astype(jnp.float32)
    own_weight = lax.optimization_barrier((own_exponent / denominator).astype(jnp.bfloat16)).astype(jnp.float32)
    combined = jnp.einsum('bkgc,bckd->bkgd', weights, value_four)
    combined = combined + own_weight[..., None] * own_value[:, :, None, :]
    return combined.reshape(row_denominator_sum, -1).astype(jnp.bfloat16)

def reference(queries, new_keys, new_values, key_cache, value_cache, context_len, cache_slot, residual_in, out_weight, gate_weight, up_weight):
    block_count = ROWS // ROWS_DEV

    def one_block(block_index):
        row_start = (block_index * ROWS_DEV).astype(jnp.int32)
        slot_rows = lax.dynamic_slice_in_dim(cache_slot, row_start, ROWS_DEV)
        key_rows = jnp.take(key_cache, slot_rows, axis=0)
        value_rows = jnp.take(value_cache, slot_rows, axis=0)
        return attend_block(lax.dynamic_slice_in_dim(queries, row_start, ROWS_DEV), lax.dynamic_slice_in_dim(new_keys, row_start, ROWS_DEV), lax.dynamic_slice_in_dim(new_values, row_start, ROWS_DEV), key_rows, value_rows, lax.dynamic_slice_in_dim(context_len, row_start, ROWS_DEV))
    attended = lax.map(one_block, jnp.arange(block_count, dtype=jnp.int32))
    attended = attended.reshape(ROWS, H * HD)
    output_projected = jnp.dot(attended, out_weight, preferred_element_type=jnp.float32)
    residual_out = (residual_in.astype(jnp.float32) + output_projected).astype(jnp.bfloat16)
    widened = lax.optimization_barrier(residual_out).astype(jnp.float32)
    squares = lax.optimization_barrier(jnp.sum(widened * widened, axis=1))
    inverse_rms = lax.rsqrt(squares / D + norm_epsilon)
    gate_value = jnp.dot(residual_out, gate_weight, preferred_element_type=jnp.float32) * inverse_rms[:, None]
    upward = jnp.dot(residual_out, up_weight, preferred_element_type=jnp.float32) * inverse_rms[:, None]
    activation = (jax.nn.silu(gate_value) * upward).astype(jnp.bfloat16)
    return (residual_out, activation)
```

```python
import functools

import jax
import jax.numpy as jnp
from jax import lax
from jax.experimental import pallas as pl
from jax.experimental.pallas import tpu as pltpu
from jax.sharding import PartitionSpec as P

D = 8192
HD = 128


norm_epsilon = 1e-05
masked_score = -1e30


def attend_rows(queries, new_keys, new_values, key_rows, value_rows, context_len):
    row_denominator_sum = queries.shape[0]
    context = key_rows.shape[1]
    kv_heads = key_rows.shape[2] // HD
    groups = queries.shape[1] // key_rows.shape[2]
    attention_logit_scale = HD ** (-0.5)
    query_grouped_four = queries.reshape(row_denominator_sum, kv_heads, groups, HD)
    key_four = key_rows.reshape(row_denominator_sum, context, kv_heads, HD)
    value_four = value_rows.reshape(row_denominator_sum, context, kv_heads, HD)
    current_key = new_keys.reshape(row_denominator_sum, kv_heads, HD)
    own_value = new_values.reshape(row_denominator_sum, kv_heads, HD).astype(jnp.float32)
    scores = (
        jnp.einsum(
            "bkgd,bckd->bkgc", query_grouped_four, key_four, preferred_element_type=jnp.float32
        )
        * attention_logit_scale
    )
    positions = jnp.arange(context, dtype=jnp.int32)
    valid_mask = positions[None, :] < context_len[:, None]
    scores = jnp.where(valid_mask[:, None, None, :], scores, masked_score)
    current_score = (
        jnp.einsum(
            "cnhz,cnz->cnh", query_grouped_four, current_key, preferred_element_type=jnp.float32
        )
        * attention_logit_scale
    )
    row_max = jnp.maximum(jnp.max(scores, axis=3), current_score)
    exponent = jnp.exp(scores - row_max[..., None])
    own_exponent = jnp.exp(current_score - row_max)
    denominator = jnp.sum(exponent, axis=3) + own_exponent
    weights = (exponent / denominator[..., None]).astype(jnp.bfloat16)
    own_weight = (own_exponent / denominator).astype(jnp.bfloat16).astype(jnp.float32)
    combined = jnp.einsum(
        "bkgc,bckd->bkgd", weights, value_four, preferred_element_type=jnp.float32
    )
    combined = combined + own_weight[..., None] * own_value[:, :, None, :]
    return combined.reshape(row_denominator_sum, -1).astype(jnp.bfloat16)


MESH = pl.DeviceIdType.MESH
SUBS = 4


def remote(src, dst, send_sem, recv_sem, device):
    return pltpu.make_async_remote_copy(
        src_ref=src,
        dst_ref=dst,
        send_sem=send_sem,
        recv_sem=recv_sem,
        device_id=device,
        device_id_type=MESH,
    )


def layer_kernel(
    sizes,
    att,
    res_in,
    w_hbm,
    gate_hbm,
    up_hbm,
    res_out,
    act_out,
    w_buf,
    gate_buf,
    up_buf,
    res_peer,
    disp,
    feats,
    acc,
    rs_send,
    rs_recv,
    xg,
    squares,
    sq_send,
    sq_recv,
    result,
    keep,
    ex_send,
    ex_recv,
    load_sem,
    peer_send_sem,
    peer_recv_sem,
    disp_send_sem,
    disp_recv_sem,
    fwd_send_sem,
    fwd_recv_sem,
    rs_send_sem,
    rs_recv_sem,
    ag_send_sem,
    ag_recv_sem,
    half_send_sem,
    half_recv_sem,
    sq_send_sem,
    sq_recv_sem,
    ex_send_sem,
    ex_recv_sem,
):
    groups, n, parts = sizes
    h = n // 2
    g = lax.axis_index("grp")
    m = lax.axis_index("mr")
    c = lax.axis_index("mc")
    peer = (1 - g, m, c)
    rows, width = att.shape
    feat = w_hbm.shape[0]
    half = width // 2
    sub = half // SUBS
    blocks = width // feat
    tile = result.shape[3]
    tiles = act_out.shape[1] // tile
    kept = act_out.shape[0]

    def chip_at(q):
        q = lax.rem(q + 2 * n, n)
        t = q // h
        return (1 - t) * 2 * q + t * (2 * n - 1 - 2 * q)

    place = (1 - m % 2) * (m // 2) + (m % 2) * (n - 1 - m // 2)
    right = (g, chip_at(place + 1), c)
    left = (g, chip_at(place - 1), c)

    w_load = pltpu.make_async_copy(
        w_hbm.at[:, pl.ds(pl.multiple_of(g * half, half), half)], w_buf.at[g], load_sem.at[0]
    )
    gate_load = pltpu.make_async_copy(gate_hbm, gate_buf, load_sem.at[1])
    up_load = pltpu.make_async_copy(up_hbm, up_buf, load_sem.at[2])
    w_load.start()

    barrier = pltpu.get_barrier_semaphore()
    total = groups * n * parts
    me = (g * n + m) * parts + c

    def greet(i, carry):
        other = lax.rem(me + i, total)
        device = (other // (n * parts), (other // parts) % n, other % parts)
        pl.semaphore_signal(barrier, inc=1, device_id=device, device_id_type=MESH)
        return carry

    lax.fori_loop(1, total, greet, 0)
    pl.semaphore_wait(barrier, total - 1)

    pending = []
    own_slot = g * n + m

    for k in range(parts):
        for j in range(blocks):
            jj = lax.rem(m + j, blocks)
            block = c * blocks + jj
            device = (block // n, block % n, lax.rem(c + k, parts))
            copy = remote(
                att.at[:, pl.ds(pl.multiple_of(jj * feat, feat), feat)],
                disp.at[block // n, own_slot],
                disp_send_sem.at[k, j],
                disp_recv_sem.at[own_slot],
                device,
            )
            if k == 0:
                pl.when(block != own_slot)(copy.start)

                @pl.when(block == own_slot)
                def _():
                    disp[g, own_slot] = att[:, pl.ds(pl.multiple_of(jj * feat, feat), feat)]

                pending.append((copy, block != own_slot))
            else:
                copy.start()
                pending.append((copy, None))

    other_cols = pl.ds(pl.multiple_of((1 - g) * half, half), half)
    own_cols = pl.ds(pl.multiple_of(g * half, half), half)
    w_share = remote(
        w_hbm.at[:, other_cols], w_buf.at[g], peer_send_sem.at[0], peer_recv_sem.at[0], peer
    )
    w_share.start()
    res_share = remote(
        res_in.at[:, other_cols], res_peer, peer_send_sem.at[1], peer_recv_sem.at[1], peer
    )
    res_share.start()
    pending += [(w_share, None), (res_share, None)]
    gate_load.start()
    up_load.start()

    source = own_slot // blocks
    from_self = c == source
    for i in range(groups * n):
        arrived = remote(
            disp.at[g, i], disp.at[g, i], disp_send_sem.at[0, 0], disp_recv_sem.at[i], peer
        )
        is_remote = jnp.logical_or(source != c, own_slot != i)
        pl.when(is_remote)(arrived.wait_recv)
        forward = remote(
            disp.at[g, i], disp.at[g, i], fwd_send_sem.at[i], fwd_recv_sem.at[i], peer
        )
        forward.start()
        pending.append((forward, None))
    for i in range(groups * n):
        remote(
            disp.at[1 - g, i], disp.at[1 - g, i], fwd_send_sem.at[i], fwd_recv_sem.at[i], peer
        ).wait_recv()
    for i in range(n):
        for k in range(groups):
            pair = [disp[k, gg * n + i].astype(jnp.float32) for gg in range(groups)]
            feats[i, :, k * feat : (k + 1) * feat] = jnp.concatenate(pair, axis=0).astype(
                jnp.bfloat16
            )
    w_load.wait()
    w_share.wait_recv()
    res_share.wait_recv()

    step_cols = min(512, half)

    def project(t, carry):
        cols = pl.ds(pl.multiple_of(t * step_cols, step_cols), step_cols)
        value = jnp.dot(
            feats[...].reshape(n * groups * rows, groups * feat),
            w_buf[:, :, cols].reshape(groups * feat, step_cols),
            preferred_element_type=jnp.float32,
        )
        acc[:, :, cols] = value.reshape(n, groups * rows, step_cols)
        return carry

    lax.fori_loop(0, half // step_cols, project, 0)

    def travels(direction, k):
        return (k < SUBS // 2) == (direction == 0)

    def rs_copy(direction, s, k):
        cols = pl.ds(k * sub, sub)
        return remote(
            rs_send.at[direction, s, :, cols],
            rs_recv.at[direction, s, :, cols],
            rs_send_sem.at[direction, s, k],
            rs_recv_sem.at[direction, s, k],
            right if direction == 0 else left,
        )

    for s in range(h):
        for k in range(SUBS):
            for direction in range(2):
                if s == 0 and not travels(direction, k):
                    continue
                cols = pl.ds(k * sub, sub)
                goal = chip_at(place + h - s if direction == 0 else place - h + s)
                value = acc[goal, :, cols]
                if s > 1 or (s == 1 and travels(direction, k)):
                    rs_copy(direction, s - 1, k).wait_recv()
                    value = value + rs_recv[direction, s - 1, :, cols].astype(jnp.float32)
                rs_send[direction, s, :, cols] = value.astype(jnp.bfloat16)
                copy = rs_copy(direction, s, k)
                copy.start()
                pending.append((copy, None))

    def ag_copy(direction, s, k, holder):
        cols = pl.ds(pl.multiple_of(g * half + k * sub, sub), sub)
        return remote(
            xg.at[holder, :, cols],
            xg.at[holder, :, cols],
            ag_send_sem.at[direction, s, k],
            ag_recv_sem.at[direction, s, k],
            right if direction == 0 else left,
        )

    def half_copy(holder, side, slot, k):
        cols = pl.ds(pl.multiple_of(side * half + k * sub, sub), sub)
        return remote(
            xg.at[holder, :, cols],
            xg.at[holder, :, cols],
            half_send_sem.at[slot, k],
            half_recv_sem.at[slot, k],
            peer,
        )

    def add_squares(holder):
        wide = xg[holder].astype(jnp.float32)
        summed = jnp.sum(wide * wide, axis=1, keepdims=True)
        squares[holder] = jnp.broadcast_to(summed, (groups * rows, 128)).reshape(groups, rows, 128)

    for k in range(SUBS):
        cols = pl.ds(k * sub, sub)
        for direction in range(2):
            rs_copy(direction, h - 1, k).wait_recv()
        mine = res_in[:, pl.ds(pl.multiple_of(g * half + k * sub, sub), sub)].astype(jnp.float32)
        other = res_peer[:, cols].astype(jnp.float32)
        first = jnp.where(g == 0, mine, other)
        second = jnp.where(g == 0, other, mine)
        value = acc[m, :, cols]
        for direction in range(2):
            value = value + rs_recv[direction, h - 1, :, cols].astype(jnp.float32)
        value = value + jnp.concatenate([first, second], axis=0)
        xg[m, :, pl.ds(pl.multiple_of(g * half + k * sub, sub), sub)] = value.astype(jnp.bfloat16)
        for direction in range(2):
            if h > 1 or travels(direction, k):
                copy = ag_copy(direction, 0, k, m)
                copy.start()
                pending.append((copy, None))
        copy = half_copy(m, g, 0, k)
        copy.start()
        pending.append((copy, None))

    def finish(slots):
        for holder, slot in slots:
            for k in range(SUBS):
                half_copy(holder, 1 - g, slot, k).wait_recv()
            add_squares(holder)

    waiting = [(m, 0)]
    for s in range(h):
        arrivals = []
        for k in range(SUBS):
            for direction in range(2):
                last = s == h - 1
                if last and not travels(direction, k):
                    continue
                holder = chip_at(place - 1 - s if direction == 0 else place + 1 + s)
                slot = n - 1 if last else 1 + 2 * s + direction
                ag_copy(direction, s, k, holder).wait_recv()
                if s + 1 < h and (s + 1 < h - 1 or travels(direction, k)):
                    copy = ag_copy(direction, s + 1, k, holder)
                    copy.start()
                    pending.append((copy, None))
                copy = half_copy(holder, g, slot, k)
                copy.start()
                pending.append((copy, None))
                if k == 0 or (last and k == SUBS // 2):
                    if not (last and arrivals):
                        arrivals.append((holder, slot))
        finish(waiting)
        waiting = arrivals
    finish(waiting)

    both = xg[m].astype(jnp.float32)
    res_out[...] = jnp.where(g == 0, both[:rows], both[rows:]).astype(jnp.bfloat16)

    per_group = parts // groups
    count = n // per_group

    def span(target):
        return pl.ds((target % per_group) * count, count), target // per_group

    def sq_copy(k):
        return remote(
            sq_send.at[k - 1],
            sq_recv.at[k - 1],
            sq_send_sem.at[k - 1],
            sq_recv_sem.at[k - 1],
            (g, m, lax.rem(c + k, parts)),
        )

    for k in range(1, parts):
        chips, group = span(lax.rem(c + k, parts))
        sq_send[k - 1] = squares[chips, group]
        copy = sq_copy(k)
        copy.start()
        pending.append((copy, None))

    gate_load.wait()
    up_load.wait()

    def ex_copy(k, w, t):
        return remote(
            ex_send.at[k - 1, w, t],
            ex_recv.at[k - 1, w, t],
            ex_send_sem.at[k - 1, w, t],
            ex_recv_sem.at[k - 1, w, t],
            (g, m, lax.rem(c + k, parts)),
        )

    def expand(t, carry):
        cols = pl.ds(pl.multiple_of(t * tile, tile), tile)
        for w, weights in enumerate((gate_buf, up_buf)):
            value = jnp.dot(
                xg[...].reshape(n * groups * rows, width),
                weights[:, cols],
                preferred_element_type=jnp.float32,
            )
            result[...] = value.reshape(n, groups, rows, tile)
            for k in range(1, parts):
                chips, group = span(lax.rem(c + k, parts))
                ex_send[k - 1, w, t] = (
                    result[chips, group].reshape(kept, tile).astype(jnp.bfloat16)
                )
                ex_copy(k, w, t).start()
            chips, group = span(c)
            keep[w, t] = result[chips, group].reshape(kept, tile)
        return carry

    lax.fori_loop(0, tiles, expand, 0)

    chips, group = span(c)
    summed = squares[chips, group]
    for k in range(1, parts):
        sq_copy(k).wait_recv()
        summed = summed + sq_recv[k - 1]
    inverse = lax.rsqrt(summed / D + norm_epsilon).reshape(kept, 128)[:, :1]

    def activate(t, carry):
        sums = []
        for w in range(2):
            value = keep[w, t]
            for k in range(1, parts):
                ex_copy(k, w, t).wait()
                value = value + ex_recv[k - 1, w, t].astype(jnp.float32)
            sums.append(value * inverse)
        gate, up = sums
        cols = pl.ds(pl.multiple_of(t * tile, tile), tile)
        act_out[:, cols] = (gate / (1.0 + jnp.exp(-gate)) * up).astype(jnp.bfloat16)
        return carry

    lax.fori_loop(0, tiles, activate, 0)

    for copy, condition in pending:
        if condition is None:
            copy.wait_send()
        else:
            pl.when(condition)(copy.wait_send)


def layer(sizes, attended, residual_in, out_weight, gate_weight, up_weight):
    groups, n, parts = sizes
    h = n // 2
    rows, width = attended.shape
    feat = out_weight.shape[0]
    half = width // 2
    hidden = gate_weight.shape[1]
    tile = 256 if hidden % 256 == 0 else 128
    tiles = hidden // tile
    kept = groups * n * rows // parts
    bf16, f32 = jnp.bfloat16, jnp.float32
    dma = pltpu.SemaphoreType.DMA
    vmem = pl.BlockSpec(memory_space=pltpu.VMEM)
    anywhere = pl.BlockSpec(memory_space=pl.ANY)
    blocks = width // feat
    return pl.pallas_call(
        functools.partial(layer_kernel, sizes),
        out_shape=(
            jax.ShapeDtypeStruct((rows, width), bf16),
            jax.ShapeDtypeStruct((kept, hidden), bf16),
        ),
        in_specs=[vmem, vmem, anywhere, anywhere, anywhere],
        out_specs=(vmem, vmem),
        scratch_shapes=[
            pltpu.VMEM((groups, feat, half), bf16),
            pltpu.VMEM(gate_weight.shape, bf16),
            pltpu.VMEM(up_weight.shape, bf16),
            pltpu.VMEM((rows, half), bf16),
            pltpu.VMEM((groups, groups * n, rows, feat), bf16),
            pltpu.VMEM((n, groups * rows, groups * feat), bf16),
            pltpu.VMEM((n, groups * rows, half), f32),
            pltpu.VMEM((2, h, groups * rows, half), bf16),
            pltpu.VMEM((2, h, groups * rows, half), bf16),
            pltpu.VMEM((n, groups * rows, width), bf16),
            pltpu.VMEM((n, groups, rows, 128), f32),
            pltpu.VMEM((parts - 1, kept // rows, rows, 128), f32),
            pltpu.VMEM((parts - 1, kept // rows, rows, 128), f32),
            pltpu.VMEM((n, groups, rows, tile), f32),
            pltpu.VMEM((2, tiles, kept, tile), f32),
            pltpu.VMEM((parts - 1, 2, tiles, kept, tile), bf16),
            pltpu.VMEM((parts - 1, 2, tiles, kept, tile), bf16),
            dma((3,)),
            dma((2,)),
            dma((2,)),
            dma((parts, blocks)),
            dma((groups * n,)),
            dma((groups * n,)),
            dma((groups * n,)),
            dma((2, h, SUBS)),
            dma((2, h, SUBS)),
            dma((2, h, SUBS)),
            dma((2, h, SUBS)),
            dma((n, SUBS)),
            dma((n, SUBS)),
            dma((parts - 1,)),
            dma((parts - 1,)),
            dma((parts - 1, 2, tiles)),
            dma((parts - 1, 2, tiles)),
        ],
        compiler_params=pltpu.CompilerParams(
            collective_id=0, has_side_effects=True, vmem_limit_bytes=67043328
        ),
    )(attended, residual_in, out_weight, gate_weight, up_weight)


def body(
    queries,
    new_keys,
    new_values,
    key_cache,
    value_cache,
    context_len,
    cache_slot,
    residual_in,
    out_weight,
    gate_weight,
    up_weight,
):
    local_rows = queries.shape[0]
    row_base = lax.axis_index(("grp", "mr")) * local_rows
    device_slot_index = cache_slot - row_base
    positions = jnp.arange(local_rows, dtype=jnp.int32)
    matches = device_slot_index[:, None] == positions[None, :]
    inverse = jnp.sum(jnp.where(matches, positions[:, None], 0), axis=0)
    by_cache = attend_rows(
        jnp.take(queries, inverse, axis=0),
        jnp.take(new_keys, inverse, axis=0),
        jnp.take(new_values, inverse, axis=0),
        key_cache,
        value_cache,
        jnp.take(context_len, inverse, axis=0),
    )
    attended = jnp.take(by_cache, device_slot_index, axis=0)
    sizes = (lax.axis_size("grp"), lax.axis_size("mr"), lax.axis_size("mc"))
    return layer(sizes, attended, residual_in, out_weight, gate_weight, up_weight)


def solution(mesh):
    in_specs = (
        P(("grp", "mr"), "mc"),
        P(("grp", "mr"), "mc"),
        P(("grp", "mr"), "mc"),
        P(("grp", "mr"), None, "mc"),
        P(("grp", "mr"), None, "mc"),
        P(("grp", "mr")),
        P(("grp", "mr")),
        P(("grp", "mr"), "mc"),
        P(("grp", "mr"), "mc"),
        P("mc", ("grp", "mr")),
        P("mc", ("grp", "mr")),
    )
    out_specs = (P(("grp", "mr"), "mc"), P("mc", ("grp", "mr")))
    return jax.shard_map(body, mesh=mesh, in_specs=in_specs, out_specs=out_specs, check_vma=False)
```

```python
import functools

import jax
import jax.numpy as jnp
from jax import lax
from jax.experimental import pallas as pl
from jax.experimental.pallas import tpu as pltpu
from jax.sharding import PartitionSpec as P

D = 8192
HD = 128


norm_epsilon = 1e-05
masked_score = -1e30


SPANS = 2
BATCH = 6
AHEAD = 3


def attend_kernel(
    lengths,
    slots,
    queries,
    new_keys,
    new_values,
    key_hbm,
    value_hbm,
    out,
    keys,
    values,
    by_head,
    out_head,
    own_keys,
    own_values,
    held,
    own_held,
    key_sem,
    value_sem,
):
    rows = queries.shape[0]
    context, width = keys.shape[1:]
    kv_heads = width // HD
    heads = queries.shape[1] // HD
    groups = heads // kv_heads
    span = context // SPANS
    scale = HD ** (-0.5)
    base = (lax.axis_index("grp") * lax.axis_size("mr") + lax.axis_index("mr")) * rows

    def copy(which, r, b):
        hbm, buffer, sem = (
            (key_hbm, keys, key_sem) if which == 0 else (value_hbm, values, value_sem)
        )
        positions = pl.ds(b * span, span)
        return pltpu.make_async_copy(
            hbm.at[slots[r] - base, positions], buffer.at[r, positions], sem.at[r, b]
        )

    def when_used(r, b, act):
        if b == 0:
            act()
        else:
            pl.when(lengths[r] > b * span)(act)

    def fetch(batch):
        for which in range(2):
            for i in range(BATCH):
                r = batch * BATCH + i
                for b in range(SPANS):
                    when_used(r, b, lambda: copy(which, r, b).start())
        for i in range(BATCH):
            r = batch * BATCH + i
            for b in range(1, SPANS):

                @pl.when(lengths[r] <= b * span)
                def _():
                    values[r, b * span : (b + 1) * span] = jnp.zeros((span, width), values.dtype)

    row_head = lax.broadcasted_iota(jnp.int32, (heads, width), 0) // groups
    column_head = lax.broadcasted_iota(jnp.int32, (heads, width), 1) // HD
    same_head = row_head == column_head

    def weigh(r):
        length = lengths[r]
        query = by_head[pl.ds(r, heads, stride=rows), :]
        spread = jnp.where(same_head, jnp.concatenate([query] * kv_heads, axis=1), 0.0)
        scores = (
            lax.dot_general(
                spread.astype(jnp.bfloat16),
                keys[r],
                (((1,), (1,)), ((), ())),
                preferred_element_type=jnp.float32,
            )
            * scale
        )
        positions = lax.broadcasted_iota(jnp.int32, (heads, context), 1)
        scores = jnp.where(positions < length, scores, masked_score)
        own_score = jnp.sum(spread * own_keys[pl.ds(r, 1), :], axis=1, keepdims=True) * scale
        top = jnp.maximum(jnp.max(scores, axis=1, keepdims=True), own_score)
        exponent = jnp.exp(scores - top)
        own_exponent = jnp.exp(own_score - top)
        denominator = jnp.sum(exponent, axis=1, keepdims=True) + own_exponent
        weights = (exponent / denominator).astype(jnp.bfloat16)
        own_weight = (own_exponent / denominator).astype(jnp.bfloat16).astype(jnp.float32)
        return weights, jnp.broadcast_to(own_weight, (heads, HD))

    def combine(r, weights, own_weight):
        combined = jnp.dot(weights, values[r], preferred_element_type=jnp.float32)
        combined = combined + own_weight[:, :1] * own_values[pl.ds(r, 1), :]
        combined = jnp.where(same_head, combined, 0.0)
        picked = combined[:, :HD]
        for k in range(1, kv_heads):
            picked = picked + combined[:, k * HD : (k + 1) * HD]
        return picked

    def weigh_batch(batch):
        return [weigh(batch * BATCH + i) for i in range(BATCH)]

    def hold(found):
        for i, (weights, own_weight) in enumerate(found):
            held[i] = weights
            own_held[i] = own_weight

    def combine_batch(batch):
        return [combine(batch * BATCH + i, held[i], own_held[i]) for i in range(BATCH)]

    def put(batch, picked):
        for i in range(BATCH):
            out_head[pl.ds(batch * BATCH + i, heads, stride=rows), :] = picked[i]

    def arrive(which, batch):
        for i in range(BATCH):
            r = batch * BATCH + i
            for b in range(SPANS):
                when_used(r, b, lambda: copy(which, r, b).wait())

    batches = rows // BATCH

    def first(batch, carry):
        fetch(batch)
        return carry

    lax.fori_loop(0, min(AHEAD, batches), first, 0)

    own_keys[...] = new_keys[...].astype(jnp.float32)
    own_values[...] = new_values[...].astype(jnp.float32)
    for j in range(heads):
        by_head[j * rows : (j + 1) * rows, :] = queries[:, j * HD : (j + 1) * HD].astype(
            jnp.float32
        )

    arrive(0, 0)
    hold(weigh_batch(0))

    def step(batch, carry):
        @pl.when(batch + AHEAD <= batches)
        def _():
            fetch(batch + AHEAD - 1)

        arrive(1, batch - 1)
        arrive(0, batch)
        picked = combine_batch(batch - 1)
        found = weigh_batch(batch)
        put(batch - 1, picked)
        hold(found)
        return carry

    lax.fori_loop(1, batches, step, 0)
    arrive(1, batches - 1)
    put(batches - 1, combine_batch(batches - 1))
    for j in range(heads):
        out[:, j * HD : (j + 1) * HD] = out_head[j * rows : (j + 1) * rows, :].astype(jnp.bfloat16)


def attend_rows(queries, new_keys, new_values, key_cache, value_cache, context_len, cache_slot):
    rows = queries.shape[0]
    _, context, width = key_cache.shape
    heads = queries.shape[1] // HD
    vmem = pl.BlockSpec(memory_space=pltpu.VMEM)
    smem = pl.BlockSpec(memory_space=pltpu.SMEM)
    hbm = pl.BlockSpec(memory_space=pltpu.HBM)
    return pl.pallas_call(
        attend_kernel,
        out_shape=jax.ShapeDtypeStruct(queries.shape, jnp.bfloat16),
        in_specs=[smem, smem, vmem, vmem, vmem, hbm, hbm],
        out_specs=vmem,
        scratch_shapes=[
            pltpu.VMEM((rows, context, width), jnp.bfloat16),
            pltpu.VMEM((rows, context, width), jnp.bfloat16),
            pltpu.VMEM((heads * rows, HD), jnp.float32),
            pltpu.VMEM((heads * rows, HD), jnp.float32),
            pltpu.VMEM((rows, width), jnp.float32),
            pltpu.VMEM((rows, width), jnp.float32),
            pltpu.VMEM((BATCH, heads, context), jnp.bfloat16),
            pltpu.VMEM((BATCH, heads, HD), jnp.float32),
            pltpu.SemaphoreType.DMA((rows, SPANS)),
            pltpu.SemaphoreType.DMA((rows, SPANS)),
        ],
        compiler_params=pltpu.CompilerParams(vmem_limit_bytes=56 * 1024 * 1024),
    )(context_len, cache_slot, queries, new_keys, new_values, key_cache, value_cache)


MESH = pl.DeviceIdType.MESH
SUBS = 4


def remote(src, dst, send_sem, recv_sem, device):
    return pltpu.make_async_remote_copy(
        src_ref=src,
        dst_ref=dst,
        send_sem=send_sem,
        recv_sem=recv_sem,
        device_id=device,
        device_id_type=MESH,
    )


def layer_kernel(
    sizes,
    att_hbm,
    res_hbm,
    w_hbm,
    gate_hbm,
    up_hbm,
    res_out_hbm,
    act_out_hbm,
    att,
    res_in,
    res_out,
    act_out,
    w_buf,
    gate_buf,
    up_buf,
    res_peer,
    disp,
    feats,
    acc,
    rs_send,
    rs_recv,
    xg,
    squares,
    sq_keep,
    sq_send,
    sq_recv,
    result,
    keep,
    ex_send,
    ex_recv,
    load_sem,
    store_sem,
    peer_send_sem,
    peer_recv_sem,
    disp_send_sem,
    disp_recv_sem,
    fwd_send_sem,
    fwd_recv_sem,
    rs_send_sem,
    rs_recv_sem,
    ag_send_sem,
    ag_recv_sem,
    half_send_sem,
    half_recv_sem,
    sq_send_sem,
    sq_recv_sem,
    ex_send_sem,
    ex_recv_sem,
):
    groups, n, parts = sizes
    h = n // 2
    g = lax.axis_index("grp")
    m = lax.axis_index("mr")
    c = lax.axis_index("mc")
    peer = (1 - g, m, c)
    rows, width = att.shape
    feat = w_hbm.shape[0]
    half = width // 2
    sub = half // SUBS
    blocks = width // feat
    tile = result.shape[4]
    tiles = act_out.shape[2] // tile

    def chip_at(q):
        q = lax.rem(q + 2 * n, n)
        t = q // h
        return (1 - t) * 2 * q + t * (2 * n - 1 - 2 * q)

    place = (1 - m % 2) * (m // 2) + (m % 2) * (n - 1 - m // 2)
    right = (g, chip_at(place + 1), c)
    left = (g, chip_at(place - 1), c)

    w_load = pltpu.make_async_copy(
        w_hbm.at[:, pl.ds(pl.multiple_of(g * half, half), half)], w_buf.at[g], load_sem.at[0]
    )
    gate_load = pltpu.make_async_copy(gate_hbm, gate_buf, load_sem.at[1])
    up_load = pltpu.make_async_copy(up_hbm, up_buf, load_sem.at[2])
    att_load = pltpu.make_async_copy(att_hbm, att, load_sem.at[3])
    res_load = pltpu.make_async_copy(res_hbm, res_in, load_sem.at[4])
    att_load.start()
    res_load.start()
    w_load.start()

    barrier = pltpu.get_barrier_semaphore()
    total = groups * n * parts
    me = (g * n + m) * parts + c

    def greet(i, carry):
        other = lax.rem(me + i, total)
        device = (other // (n * parts), (other // parts) % n, other % parts)
        pl.semaphore_signal(barrier, inc=1, device_id=device, device_id_type=MESH)
        return carry

    lax.fori_loop(1, total, greet, 0)
    pl.semaphore_wait(barrier, total - 1)

    pending = []
    own_slot = g * n + m
    att_load.wait()
    res_load.wait()

    for k in range(parts):
        for j in range(blocks):
            jj = lax.rem(m + j, blocks)
            block = c * blocks + jj
            device = (block // n, block % n, lax.rem(c + k, parts))
            copy = remote(
                att.at[:, pl.ds(pl.multiple_of(jj * feat, feat), feat)],
                disp.at[block // n, own_slot],
                disp_send_sem.at[k, j],
                disp_recv_sem.at[own_slot],
                device,
            )
            if k == 0:
                pl.when(block != own_slot)(copy.start)

                @pl.when(block == own_slot)
                def _():
                    disp[g, own_slot] = att[:, pl.ds(pl.multiple_of(jj * feat, feat), feat)]

                pending.append((copy, block != own_slot))
            else:
                copy.start()
                pending.append((copy, None))

    other_cols = pl.ds(pl.multiple_of((1 - g) * half, half), half)
    own_cols = pl.ds(pl.multiple_of(g * half, half), half)
    w_share = remote(
        w_hbm.at[:, other_cols], w_buf.at[g], peer_send_sem.at[0], peer_recv_sem.at[0], peer
    )
    w_share.start()
    res_share = remote(
        res_in.at[:, other_cols], res_peer, peer_send_sem.at[1], peer_recv_sem.at[1], peer
    )
    res_share.start()
    pending += [(w_share, None), (res_share, None)]
    gate_load.start()
    up_load.start()

    source = own_slot // blocks
    from_self = c == source
    for i in range(groups * n):
        arrived = remote(
            disp.at[g, i], disp.at[g, i], disp_send_sem.at[0, 0], disp_recv_sem.at[i], peer
        )
        is_remote = jnp.logical_or(source != c, own_slot != i)
        pl.when(is_remote)(arrived.wait_recv)
        forward = remote(
            disp.at[g, i], disp.at[g, i], fwd_send_sem.at[i], fwd_recv_sem.at[i], peer
        )
        forward.start()
        pending.append((forward, None))
    for i in range(groups * n):
        remote(
            disp.at[1 - g, i], disp.at[1 - g, i], fwd_send_sem.at[i], fwd_recv_sem.at[i], peer
        ).wait_recv()
    for i in range(n):
        for k in range(groups):
            pair = [disp[k, gg * n + i].astype(jnp.float32) for gg in range(groups)]
            feats[i, :, k * feat : (k + 1) * feat] = jnp.concatenate(pair, axis=0).astype(
                jnp.bfloat16
            )
    w_load.wait()
    w_share.wait_recv()
    res_share.wait_recv()

    step_cols = min(512, half)

    def project(t, carry):
        cols = pl.ds(pl.multiple_of(t * step_cols, step_cols), step_cols)
        value = jnp.dot(
            feats[...].reshape(n * groups * rows, groups * feat),
            w_buf[:, :, cols].reshape(groups * feat, step_cols),
            preferred_element_type=jnp.float32,
        )
        acc[:, :, cols] = value.reshape(n, groups * rows, step_cols)
        return carry

    lax.fori_loop(0, half // step_cols, project, 0)

    def travels(direction, k):
        return (k < SUBS // 2) == (direction == 0)

    def rs_copy(direction, s, k):
        cols = pl.ds(k * sub, sub)
        return remote(
            rs_send.at[direction, s, :, cols],
            rs_recv.at[direction, s, :, cols],
            rs_send_sem.at[direction, s, k],
            rs_recv_sem.at[direction, s, k],
            right if direction == 0 else left,
        )

    for s in range(h):
        for turn in range(SUBS):
            for direction in range(2):
                k = (turn + SUBS // 2) % SUBS if direction == 0 else turn
                if s == 0 and not travels(direction, k):
                    continue
                cols = pl.ds(k * sub, sub)
                goal = chip_at(place + h - s if direction == 0 else place - h + s)
                value = acc[goal, :, cols]
                if s > 1 or (s == 1 and travels(direction, k)):
                    rs_copy(direction, s - 1, k).wait_recv()
                    value = value + rs_recv[direction, s - 1, :, cols].astype(jnp.float32)
                rs_send[direction, s, :, cols] = value.astype(jnp.bfloat16)
                copy = rs_copy(direction, s, k)
                copy.start()
                pending.append((copy, None))

    def ag_copy(direction, s, k, holder):
        cols = pl.ds(pl.multiple_of(g * half + k * sub, sub), sub)
        return remote(
            xg.at[holder, :, cols],
            xg.at[holder, :, cols],
            ag_send_sem.at[direction, s, k],
            ag_recv_sem.at[direction, s, k],
            right if direction == 0 else left,
        )

    def half_copy(holder, side, slot, k):
        cols = pl.ds(pl.multiple_of(side * half + k * sub, sub), sub)
        return remote(
            xg.at[holder, :, cols],
            xg.at[holder, :, cols],
            half_send_sem.at[slot, k],
            half_recv_sem.at[slot, k],
            peer,
        )

    for k in range(SUBS):
        cols = pl.ds(k * sub, sub)
        mine = res_in[:, pl.ds(pl.multiple_of(g * half + k * sub, sub), sub)].astype(jnp.float32)
        other = res_peer[:, cols].astype(jnp.float32)
        first = jnp.where(g == 0, mine, other)
        second = jnp.where(g == 0, other, mine)
        value = acc[m, :, cols] + jnp.concatenate([first, second], axis=0)
        for direction in range(2):
            rs_copy(direction, h - 1, k).wait_recv()
            value = value + rs_recv[direction, h - 1, :, cols].astype(jnp.float32)
        xg[m, :, pl.ds(pl.multiple_of(g * half + k * sub, sub), sub)] = value.astype(jnp.bfloat16)
        copy = half_copy(m, g, 0, k)
        copy.start()
        pending.append((copy, None))
        if h > 1 or travels(0, k):
            copy = ag_copy(0, 0, k, m)
            copy.start()
            pending.append((copy, None))

    for turn in range(SUBS):
        k = (turn + SUBS // 2) % SUBS
        if h > 1 or travels(1, k):
            copy = ag_copy(1, 0, k, m)
            copy.start()
            pending.append((copy, None))

    order = [m]
    for s in range(h - 1):
        order += [chip_at(place - 1 - s), chip_at(place + 1 + s)]
    order.append(chip_at(place + h))
    stages = [(0, 1)] + [(1 + 2 * s, 2) for s in range(h - 1)] + [(n - 1, 1)]
    per_group = parts // groups
    count = n // per_group
    own_group = c // per_group

    def keeper(group, holder):
        return group * per_group + holder // count

    def slot_of(source, target):
        return 0 if parts == 2 else lax.rem(source - target + parts, parts) - 1

    def ex_copy(source, target, stage, t):
        first, size = stage
        where = (slot_of(source, target), t, slice(None), pl.ds(first, size))
        return remote(
            ex_send.at[where],
            ex_recv.at[where],
            ex_send_sem.at[slot_of(source, target), t, first],
            ex_recv_sem.at[slot_of(source, target), t, first],
            (g, m, target),
        )

    def sq_copy(source, target, stage):
        first, size = stage
        where = (slot_of(source, target), pl.ds(first, size))
        return remote(
            sq_send.at[where],
            sq_recv.at[where],
            sq_send_sem.at[slot_of(source, target), first],
            sq_recv_sem.at[slot_of(source, target), first],
            (g, m, target),
        )

    def items(stage):
        first, size = stage
        if per_group == 1:
            return [stage]
        return [(first + i, 1) for i in range(size)]

    def mine_to_keep(j, item):
        if j > 0:
            return False, None
        if per_group == 1:
            return True, None
        return None, order[item[0]] // count == lax.rem(c, per_group)

    def pack_squares(column):
        lane = lax.broadcasted_iota(jnp.int32, (8, 128), 1)
        packed = jnp.zeros((8, 128), jnp.float32)
        for a in range(rows // 8):
            packed = packed + jnp.where(lane == a, column[8 * a : 8 * a + 8], 0.0)
        return packed

    def route(j, item, keep_it, send_it):
        certain, condition = mine_to_keep(j, item)
        if certain is None:
            pl.when(condition)(keep_it)
            pl.when(jnp.logical_not(condition))(send_it)
        elif certain:
            keep_it()
        else:
            send_it()

    def run_stage(stage):
        first, size = stage
        for i in range(first, first + size):
            wide = xg[order[i]].astype(jnp.float32)
            summed = jnp.sum(wide * wide, axis=1, keepdims=True)
            squares[i] = jnp.broadcast_to(summed, (groups * rows, 128)).reshape(groups, rows, 128)
        for item in items(stage):
            for j in range(groups):
                group = lax.rem(own_group + j, groups)
                target = keeper(group, order[item[0]])

                def keep_it(item=item, group=group):
                    for i in range(item[0], item[0] + item[1]):
                        sq_keep[i] = pack_squares(squares[i, group])

                def send_it(item=item, group=group, target=target):
                    for i in range(item[0], item[0] + item[1]):
                        sq_send[slot_of(c, target), i] = pack_squares(squares[i, group])
                    sq_copy(c, target, item).start()

                route(j, item, keep_it, send_it)

        def expand(t, carry):
            cols = pl.ds(pl.multiple_of(t * tile, tile), tile)
            lhs = jnp.concatenate([xg[order[i]] for i in range(first, first + size)], axis=0)
            for w, weights in enumerate((gate_buf, up_buf)):
                value = jnp.dot(lhs, weights[:, cols], preferred_element_type=jnp.float32)
                result[w, :size] = value.reshape(size, groups, rows, tile)
            for item in items(stage):
                local = pl.ds(item[0] - first, item[1])
                for j in range(groups):
                    group = lax.rem(own_group + j, groups)
                    target = keeper(group, order[item[0]])

                    def keep_it(item=item, local=local, group=group):
                        keep[t, :, pl.ds(item[0], item[1])] = result[:, local, group]

                    def send_it(item=item, local=local, group=group, target=target):
                        ex_send[slot_of(c, target), t, :, pl.ds(item[0], item[1])] = result[
                            :, local, group
                        ].astype(jnp.bfloat16)
                        ex_copy(c, target, item, t).start()

                    route(j, item, keep_it, send_it)
            return carry

        lax.fori_loop(0, tiles, expand, 0)

    gate_load.wait()
    up_load.wait()
    res_store = pltpu.make_async_copy(res_out, res_out_hbm, load_sem.at[5])
    for s in range(-1, h):
        for turn in range(SUBS):
            if s < 0:
                break
            for direction in range(2):
                k = turn if direction == 0 else (turn + SUBS // 2) % SUBS
                last = s == h - 1
                if last and not travels(direction, k):
                    continue
                holder = chip_at(place - 1 - s if direction == 0 else place + 1 + s)
                slot = n - 1 if last else 1 + 2 * s + direction
                ag_copy(direction, s, k, holder).wait_recv()
                if s + 1 < h and (s + 1 < h - 1 or travels(direction, k)):
                    copy = ag_copy(direction, s + 1, k, holder)
                    copy.start()
                    pending.append((copy, None))
                copy = half_copy(holder, g, slot, k)
                copy.start()
                pending.append((copy, None))
        stage = stages[s + 1]
        for i in range(stage[0], stage[0] + stage[1]):
            for k in range(SUBS):
                half_copy(order[i], 1 - g, i, k).wait_recv()
        if s < 0:
            both = xg[m].astype(jnp.float32)
            res_out[...] = jnp.where(g == 0, both[:rows], both[rows:]).astype(jnp.bfloat16)
            res_store.start()
        run_stage(stage)

    def finish(item):
        total = [sq_keep[i] for i in range(item[0], item[0] + item[1])]
        for k in range(1, parts):
            source = lax.rem(c + k, parts)
            sq_copy(source, c, item).wait_recv()
            total = [
                value + sq_recv[slot_of(source, c), item[0] + i] for i, value in enumerate(total)
            ]
        inverse = []
        for value in total:
            packed = lax.rsqrt(value / D + norm_epsilon)
            inverse.append(
                jnp.concatenate([packed[:, a : a + 1] for a in range(rows // 8)], axis=0)
            )

        def activate(t, carry):
            for k in range(1, parts):
                ex_copy(lax.rem(c + k, parts), c, item, t).wait_recv()
            cols = pl.ds(pl.multiple_of(t * tile, tile), tile)
            for i, scale in enumerate(inverse):
                sums = []
                for w in range(2):
                    value = keep[t, w, item[0] + i]
                    for k in range(1, parts):
                        slot = slot_of(lax.rem(c + k, parts), c)
                        value = value + ex_recv[slot, t, w, item[0] + i].astype(jnp.float32)
                    sums.append(value * scale)
                gate, up = sums
                holder = order[item[0] + i]
                act_out[lax.rem(holder, count), :, cols] = (
                    gate / (1.0 + jnp.exp(-gate)) * up
                ).astype(jnp.bfloat16)
            return carry

        lax.fori_loop(0, tiles, activate, 0)
        for i in range(item[0], item[0] + item[1]):
            store(lax.rem(order[i], count)).start()

    def store(index):
        return pltpu.make_async_copy(
            act_out.at[index], act_out_hbm.at[index], store_sem.at[index]
        )

    def sent(item, target):
        sq_copy(c, target, item).wait_send()

        def each(t, carry):
            ex_copy(c, target, item, t).wait_send()
            return carry

        lax.fori_loop(0, tiles, each, 0)

    for stage in stages:
        for item in items(stage):
            route(0, item, functools.partial(finish, item), lambda: None)
            for j in range(groups):
                target = keeper(lax.rem(own_group + j, groups), order[item[0]])
                route(j, item, lambda: None, functools.partial(sent, item, target))

    res_store.wait()
    for i in range(count):
        store(i).wait()
    for copy, condition in pending:
        if condition is None:
            copy.wait_send()
        else:
            pl.when(condition)(copy.wait_send)


def layer(sizes, attended, residual_in, out_weight, gate_weight, up_weight):
    groups, n, parts = sizes
    h = n // 2
    rows, width = attended.shape
    feat = out_weight.shape[0]
    half = width // 2
    hidden = gate_weight.shape[1]
    tile = hidden // 2 if hidden % 256 == 0 else 128
    tiles = hidden // tile
    kept = groups * n * rows // parts
    bf16, f32 = jnp.bfloat16, jnp.float32
    dma = pltpu.SemaphoreType.DMA
    hbm = pl.BlockSpec(memory_space=pltpu.HBM)
    blocks = width // feat
    residual_out, activation = pl.pallas_call(
        functools.partial(layer_kernel, sizes),
        out_shape=(
            jax.ShapeDtypeStruct((rows, width), bf16),
            jax.ShapeDtypeStruct((kept // rows, rows, hidden), bf16),
        ),
        in_specs=[hbm] * 5,
        out_specs=(hbm, hbm),
        scratch_shapes=[
            pltpu.VMEM((rows, width), bf16),
            pltpu.VMEM((rows, width), bf16),
            pltpu.VMEM((rows, width), bf16),
            pltpu.VMEM((kept // rows, rows, hidden), bf16),
            pltpu.VMEM((groups, feat, half), bf16),
            pltpu.VMEM(gate_weight.shape, bf16),
            pltpu.VMEM(up_weight.shape, bf16),
            pltpu.VMEM((rows, half), bf16),
            pltpu.VMEM((groups, groups * n, rows, feat), bf16),
            pltpu.VMEM((n, groups * rows, groups * feat), bf16),
            pltpu.VMEM((n, groups * rows, half), f32),
            pltpu.VMEM((2, h, groups * rows, half), bf16),
            pltpu.VMEM((2, h, groups * rows, half), bf16),
            pltpu.VMEM((n, groups * rows, width), bf16),
            pltpu.VMEM((n, groups, rows, 128), f32),
            pltpu.VMEM((n, 8, 128), f32),
            pltpu.VMEM((parts - 1, n, 8, 128), f32),
            pltpu.VMEM((parts - 1, n, 8, 128), f32),
            pltpu.VMEM((2, 2, groups, rows, tile), f32),
            pltpu.VMEM((tiles, 2, n, rows, tile), f32),
            pltpu.VMEM((parts - 1, tiles, 2, n, rows, tile), bf16),
            pltpu.VMEM((parts - 1, tiles, 2, n, rows, tile), bf16),
            dma((6,)),
            dma((kept // rows,)),
            dma((2,)),
            dma((2,)),
            dma((parts, blocks)),
            dma((groups * n,)),
            dma((groups * n,)),
            dma((groups * n,)),
            dma((2, h, SUBS)),
            dma((2, h, SUBS)),
            dma((2, h, SUBS)),
            dma((2, h, SUBS)),
            dma((n, SUBS)),
            dma((n, SUBS)),
            dma((parts - 1, n)),
            dma((parts - 1, n)),
            dma((parts - 1, tiles, n)),
            dma((parts - 1, tiles, n)),
        ],
        compiler_params=pltpu.CompilerParams(
            collective_id=0, has_side_effects=True, vmem_limit_bytes=56 * 1024 * 1024
        ),
    )(attended, residual_in, out_weight, gate_weight, up_weight)
    residual_out, activation = hand_over(residual_out, activation)
    return residual_out, activation.reshape(kept, hidden)


def hand_over_kernel(res_in, act_in, res_out, act_out, res_buf, act_buf, in_sem, out_sem):
    chips = act_in.shape[0]
    moves = [
        (
            pltpu.make_async_copy(res_in, res_buf, in_sem.at[chips]),
            pltpu.make_async_copy(res_buf, res_out, out_sem.at[chips]),
        )
    ]
    for i in range(chips):
        moves.append(
            (
                pltpu.make_async_copy(act_in.at[i], act_buf.at[i], in_sem.at[i]),
                pltpu.make_async_copy(act_buf.at[i], act_out.at[i], out_sem.at[i]),
            )
        )
    for into, _ in moves:
        into.start()
    for into, out in moves:
        into.wait()
        out.start()
    for _, out in moves:
        out.wait()


def hand_over(residual_out, activation):
    hbm = pl.BlockSpec(memory_space=pltpu.HBM)
    dma = pltpu.SemaphoreType.DMA((activation.shape[0] + 1,))
    return pl.pallas_call(
        hand_over_kernel,
        out_shape=tuple(
            jax.ShapeDtypeStruct(x.shape, x.dtype) for x in (residual_out, activation)
        ),
        in_specs=[hbm, hbm],
        out_specs=(hbm, hbm),
        scratch_shapes=[
            pltpu.VMEM(residual_out.shape, residual_out.dtype),
            pltpu.VMEM(activation.shape, activation.dtype),
            dma,
            dma,
        ],
        compiler_params=pltpu.CompilerParams(vmem_limit_bytes=56 * 1024 * 1024),
    )(residual_out, activation)


def body(
    queries,
    new_keys,
    new_values,
    key_cache,
    value_cache,
    context_len,
    cache_slot,
    residual_in,
    out_weight,
    gate_weight,
    up_weight,
):
    attended = attend_rows(
        queries, new_keys, new_values, key_cache, value_cache, context_len, cache_slot
    )
    sizes = (lax.axis_size("grp"), lax.axis_size("mr"), lax.axis_size("mc"))
    return layer(sizes, attended, residual_in, out_weight, gate_weight, up_weight)


def solution(mesh):
    in_specs = (
        P(("grp", "mr"), "mc"),
        P(("grp", "mr"), "mc"),
        P(("grp", "mr"), "mc"),
        P(("grp", "mr"), None, "mc"),
        P(("grp", "mr"), None, "mc"),
        P(("grp", "mr")),
        P(("grp", "mr")),
        P(("grp", "mr"), "mc"),
        P(("grp", "mr"), "mc"),
        P("mc", ("grp", "mr")),
        P("mc", ("grp", "mr")),
    )
    out_specs = (P(("grp", "mr"), "mc"), P("mc", ("grp", "mr")))
    return jax.shard_map(body, mesh=mesh, in_specs=in_specs, out_specs=out_specs, check_vma=False)
```

```python
import functools

import jax
import jax.numpy as jnp
from jax import lax
from jax.experimental import pallas as pl
from jax.experimental.pallas import tpu as pltpu
from jax.sharding import PartitionSpec as P

D = 8192
HD = 128


norm_epsilon = 1e-05
masked_score = -1e30


SPANS = 2
BATCH = 6
AHEAD = 3


def attend_kernel(
    lengths,
    slots,
    queries,
    new_keys,
    new_values,
    key_hbm,
    value_hbm,
    out,
    keys,
    values,
    by_head,
    out_head,
    own_keys,
    own_values,
    held,
    own_held,
    key_sem,
    value_sem,
):
    rows = queries.shape[0]
    context, width = keys.shape[1:]
    kv_heads = width // HD
    heads = queries.shape[1] // HD
    groups = heads // kv_heads
    span = context // SPANS
    scale = HD ** (-0.5)
    base = (lax.axis_index("grp") * lax.axis_size("mr") + lax.axis_index("mr")) * rows

    def copy(which, r, b):
        hbm, buffer, sem = (
            (key_hbm, keys, key_sem) if which == 0 else (value_hbm, values, value_sem)
        )
        positions = pl.ds(b * span, span)
        return pltpu.make_async_copy(
            hbm.at[slots[r] - base, positions], buffer.at[r, positions], sem.at[r, b]
        )

    def when_used(r, b, act):
        if b == 0:
            act()
        else:
            pl.when(lengths[r] > b * span)(act)

    def fetch(batch):
        for which in range(2):
            for i in range(BATCH):
                r = batch * BATCH + i
                for b in range(SPANS):
                    when_used(r, b, lambda: copy(which, r, b).start())
        for i in range(BATCH):
            r = batch * BATCH + i
            for b in range(1, SPANS):

                @pl.when(lengths[r] <= b * span)
                def _():
                    values[r, b * span : (b + 1) * span] = jnp.zeros((span, width), values.dtype)

    row_head = lax.broadcasted_iota(jnp.int32, (heads, width), 0) // groups
    column_head = lax.broadcasted_iota(jnp.int32, (heads, width), 1) // HD
    same_head = row_head == column_head

    def weigh(r):
        length = lengths[r]
        query = by_head[pl.ds(r, heads, stride=rows), :]
        spread = jnp.where(same_head, jnp.concatenate([query] * kv_heads, axis=1), 0.0)
        scores = (
            lax.dot_general(
                spread.astype(jnp.bfloat16),
                keys[r],
                (((1,), (1,)), ((), ())),
                preferred_element_type=jnp.float32,
            )
            * scale
        )
        positions = lax.broadcasted_iota(jnp.int32, (heads, context), 1)
        scores = jnp.where(positions < length, scores, masked_score)
        own_score = jnp.sum(spread * own_keys[pl.ds(r, 1), :], axis=1, keepdims=True) * scale
        top = jnp.maximum(jnp.max(scores, axis=1, keepdims=True), own_score)
        exponent = jnp.exp(scores - top)
        own_exponent = jnp.exp(own_score - top)
        denominator = jnp.sum(exponent, axis=1, keepdims=True) + own_exponent
        weights = (exponent / denominator).astype(jnp.bfloat16)
        own_weight = (own_exponent / denominator).astype(jnp.bfloat16).astype(jnp.float32)
        return weights, jnp.broadcast_to(own_weight, (heads, HD))

    def combine(r, weights, own_weight):
        combined = jnp.dot(weights, values[r], preferred_element_type=jnp.float32)
        combined = combined + own_weight[:, :1] * own_values[pl.ds(r, 1), :]
        combined = jnp.where(same_head, combined, 0.0)
        picked = combined[:, :HD]
        for k in range(1, kv_heads):
            picked = picked + combined[:, k * HD : (k + 1) * HD]
        return picked

    def weigh_batch(batch):
        return [weigh(batch * BATCH + i) for i in range(BATCH)]

    def hold(found):
        for i, (weights, own_weight) in enumerate(found):
            held[i] = weights
            own_held[i] = own_weight

    def combine_batch(batch):
        return [combine(batch * BATCH + i, held[i], own_held[i]) for i in range(BATCH)]

    def put(batch, picked):
        for i in range(BATCH):
            out_head[pl.ds(batch * BATCH + i, heads, stride=rows), :] = picked[i]

    def arrive(which, batch):
        for i in range(BATCH):
            r = batch * BATCH + i
            for b in range(SPANS):
                when_used(r, b, lambda: copy(which, r, b).wait())

    batches = rows // BATCH

    def first(batch, carry):
        fetch(batch)
        return carry

    lax.fori_loop(0, min(AHEAD, batches), first, 0)

    own_keys[...] = new_keys[...].astype(jnp.float32)
    own_values[...] = new_values[...].astype(jnp.float32)
    for j in range(heads):
        by_head[j * rows : (j + 1) * rows, :] = queries[:, j * HD : (j + 1) * HD].astype(
            jnp.float32
        )

    arrive(0, 0)
    hold(weigh_batch(0))

    def step(batch, carry):
        @pl.when(batch + AHEAD <= batches)
        def _():
            fetch(batch + AHEAD - 1)

        arrive(1, batch - 1)
        arrive(0, batch)
        picked = combine_batch(batch - 1)
        found = weigh_batch(batch)
        put(batch - 1, picked)
        hold(found)
        return carry

    lax.fori_loop(1, batches, step, 0)
    arrive(1, batches - 1)
    put(batches - 1, combine_batch(batches - 1))
    for j in range(heads):
        out[:, j * HD : (j + 1) * HD] = out_head[j * rows : (j + 1) * rows, :].astype(jnp.bfloat16)


def attend_rows(queries, new_keys, new_values, key_cache, value_cache, context_len, cache_slot):
    rows = queries.shape[0]
    _, context, width = key_cache.shape
    heads = queries.shape[1] // HD
    vmem = pl.BlockSpec(memory_space=pltpu.VMEM)
    smem = pl.BlockSpec(memory_space=pltpu.SMEM)
    hbm = pl.BlockSpec(memory_space=pltpu.HBM)
    return pl.pallas_call(
        attend_kernel,
        out_shape=jax.ShapeDtypeStruct(queries.shape, jnp.bfloat16),
        in_specs=[smem, smem, vmem, vmem, vmem, hbm, hbm],
        out_specs=vmem,
        scratch_shapes=[
            pltpu.VMEM((rows, context, width), jnp.bfloat16),
            pltpu.VMEM((rows, context, width), jnp.bfloat16),
            pltpu.VMEM((heads * rows, HD), jnp.float32),
            pltpu.VMEM((heads * rows, HD), jnp.float32),
            pltpu.VMEM((rows, width), jnp.float32),
            pltpu.VMEM((rows, width), jnp.float32),
            pltpu.VMEM((BATCH, heads, context), jnp.bfloat16),
            pltpu.VMEM((BATCH, heads, HD), jnp.float32),
            pltpu.SemaphoreType.DMA((rows, SPANS)),
            pltpu.SemaphoreType.DMA((rows, SPANS)),
        ],
        compiler_params=pltpu.CompilerParams(vmem_limit_bytes=56 * 1024 * 1024),
    )(context_len, cache_slot, queries, new_keys, new_values, key_cache, value_cache)


MESH = pl.DeviceIdType.MESH
SUBS = 4


def remote(src, dst, send_sem, recv_sem, device):
    return pltpu.make_async_remote_copy(
        src_ref=src,
        dst_ref=dst,
        send_sem=send_sem,
        recv_sem=recv_sem,
        device_id=device,
        device_id_type=MESH,
    )


def outward(count):
    return [(d + 1) // 2 if d % 2 else count - d // 2 for d in range(count)]


def layer_kernel(
    sizes,
    att_hbm,
    res_hbm,
    w_hbm,
    gate_hbm,
    up_hbm,
    res_out_hbm,
    act_out_hbm,
    att,
    res_in,
    res_out,
    act_out,
    w_buf,
    gate_buf,
    up_buf,
    res_peer,
    disp,
    feats,
    acc,
    rs_send,
    rs_recv,
    xg,
    squares,
    sq_keep,
    sq_send,
    sq_recv,
    result,
    keep,
    ex_send,
    ex_recv,
    load_sem,
    store_sem,
    peer_send_sem,
    peer_recv_sem,
    disp_send_sem,
    disp_recv_sem,
    fwd_send_sem,
    fwd_recv_sem,
    rs_send_sem,
    rs_recv_sem,
    ag_send_sem,
    ag_recv_sem,
    half_send_sem,
    half_recv_sem,
    sq_send_sem,
    sq_recv_sem,
    ex_send_sem,
    ex_recv_sem,
):
    groups, n, parts = sizes
    h = n // 2
    g = lax.axis_index("grp")
    m = lax.axis_index("mr")
    c = lax.axis_index("mc")
    peer = (1 - g, m, c)
    rows, width = att.shape
    feat = w_hbm.shape[0]
    half = width // 2
    sub = half // SUBS
    blocks = width // feat
    tile = result.shape[4]
    tiles = act_out.shape[2] // tile

    def chip_at(q):
        q = lax.rem(q + 2 * n, n)
        t = q // h
        return (1 - t) * 2 * q + t * (2 * n - 1 - 2 * q)

    place = (1 - m % 2) * (m // 2) + (m % 2) * (n - 1 - m // 2)
    right = (g, chip_at(place + 1), c)
    left = (g, chip_at(place - 1), c)

    w_load = pltpu.make_async_copy(
        w_hbm.at[:, pl.ds(pl.multiple_of(g * half, half), half)], w_buf.at[g], load_sem.at[0]
    )
    gate_load = pltpu.make_async_copy(gate_hbm, gate_buf, load_sem.at[1])
    up_load = pltpu.make_async_copy(up_hbm, up_buf, load_sem.at[2])
    att_load = pltpu.make_async_copy(att_hbm, att, load_sem.at[3])
    res_load = pltpu.make_async_copy(res_hbm, res_in, load_sem.at[4])
    att_load.start()
    res_load.start()
    w_load.start()

    barrier = pltpu.get_barrier_semaphore()
    total = groups * n * parts
    me = (g * n + m) * parts + c

    def greet(i, carry):
        other = lax.rem(me + i, total)
        device = (other // (n * parts), (other // parts) % n, other % parts)
        pl.semaphore_signal(barrier, inc=1, device_id=device, device_id_type=MESH)
        return carry

    lax.fori_loop(1, total, greet, 0)
    pl.semaphore_wait(barrier, total - 1)

    pending = []
    own_slot = g * n + m
    att_load.wait()
    res_load.wait()

    for j in range(blocks):
        for k in range(parts):
            jj = lax.rem(m + outward(blocks)[blocks - 1 - j], blocks)
            block = c * blocks + jj
            device = (block // n, block % n, lax.rem(c + k, parts))
            copy = remote(
                att.at[:, pl.ds(pl.multiple_of(jj * feat, feat), feat)],
                disp.at[block // n, own_slot],
                disp_send_sem.at[k, j],
                disp_recv_sem.at[own_slot],
                device,
            )
            if k == 0:
                pl.when(block != own_slot)(copy.start)

                @pl.when(block == own_slot)
                def _():
                    disp[g, own_slot] = att[:, pl.ds(pl.multiple_of(jj * feat, feat), feat)]

                pending.append((copy, block != own_slot))
            else:
                copy.start()
                pending.append((copy, None))

    other_cols = pl.ds(pl.multiple_of((1 - g) * half, half), half)
    own_cols = pl.ds(pl.multiple_of(g * half, half), half)
    w_share = remote(
        w_hbm.at[:, other_cols], w_buf.at[g], peer_send_sem.at[0], peer_recv_sem.at[0], peer
    )
    w_share.start()
    res_share = remote(
        res_in.at[:, other_cols], res_peer, peer_send_sem.at[1], peer_recv_sem.at[1], peer
    )
    res_share.start()
    pending += [(w_share, None), (res_share, None)]
    gate_load.start()
    up_load.start()

    source = own_slot // blocks
    for i in [gg * n + lax.rem(m + d, n) for d in outward(n) for gg in range(groups)]:
        arrived = remote(
            disp.at[g, i], disp.at[g, i], disp_send_sem.at[0, 0], disp_recv_sem.at[i], peer
        )
        is_remote = jnp.logical_or(source != c, own_slot != i)
        pl.when(is_remote)(arrived.wait_recv)
        forward = remote(
            disp.at[g, i], disp.at[g, i], fwd_send_sem.at[i], fwd_recv_sem.at[i], peer
        )
        forward.start()
        pending.append((forward, None))
    for i in range(groups * n):
        remote(
            disp.at[1 - g, i], disp.at[1 - g, i], fwd_send_sem.at[i], fwd_recv_sem.at[i], peer
        ).wait_recv()
    for i in range(n):
        for k in range(groups):
            pair = [disp[k, gg * n + i].astype(jnp.float32) for gg in range(groups)]
            feats[i, :, k * feat : (k + 1) * feat] = jnp.concatenate(pair, axis=0).astype(
                jnp.bfloat16
            )
    w_load.wait()
    w_share.wait_recv()
    res_share.wait_recv()

    step_cols = min(512, half)

    def project(t, carry):
        cols = pl.ds(pl.multiple_of(t * step_cols, step_cols), step_cols)
        value = jnp.dot(
            feats[...].reshape(n * groups * rows, groups * feat),
            w_buf[:, :, cols].reshape(groups * feat, step_cols),
            preferred_element_type=jnp.float32,
        )
        acc[:, :, cols] = value.reshape(n, groups * rows, step_cols)
        return carry

    lax.fori_loop(0, half // step_cols, project, 0)

    def travels(direction, k):
        return (k < SUBS // 2) == (direction == 0)

    def rs_copy(direction, s, k):
        cols = pl.ds(k * sub, sub)
        return remote(
            rs_send.at[direction, s, :, cols],
            rs_recv.at[direction, s, :, cols],
            rs_send_sem.at[direction, s, k],
            rs_recv_sem.at[direction, s, k],
            right if direction == 0 else left,
        )

    for s in range(h):
        for turn in range(SUBS):
            for direction in range(2):
                k = (turn + SUBS // 2) % SUBS if direction == 0 else turn
                if s == 0 and not travels(direction, k):
                    continue
                cols = pl.ds(k * sub, sub)
                goal = chip_at(place + h - s if direction == 0 else place - h + s)
                value = acc[goal, :, cols]
                if s > 1 or (s == 1 and travels(direction, k)):
                    rs_copy(direction, s - 1, k).wait_recv()
                    value = value + rs_recv[direction, s - 1, :, cols].astype(jnp.float32)
                rs_send[direction, s, :, cols] = value.astype(jnp.bfloat16)
                copy = rs_copy(direction, s, k)
                copy.start()
                pending.append((copy, None))

    def ag_copy(direction, s, k, holder):
        cols = pl.ds(pl.multiple_of(g * half + k * sub, sub), sub)
        return remote(
            xg.at[holder, :, cols],
            xg.at[holder, :, cols],
            ag_send_sem.at[direction, s, k],
            ag_recv_sem.at[direction, s, k],
            right if direction == 0 else left,
        )

    def half_copy(holder, side, slot, k):
        cols = pl.ds(pl.multiple_of(side * half + k * sub, sub), sub)
        return remote(
            xg.at[holder, :, cols],
            xg.at[holder, :, cols],
            half_send_sem.at[slot, k],
            half_recv_sem.at[slot, k],
            peer,
        )

    for k in range(SUBS):
        cols = pl.ds(k * sub, sub)
        mine = res_in[:, pl.ds(pl.multiple_of(g * half + k * sub, sub), sub)].astype(jnp.float32)
        other = res_peer[:, cols].astype(jnp.float32)
        first = jnp.where(g == 0, mine, other)
        second = jnp.where(g == 0, other, mine)
        value = acc[m, :, cols] + jnp.concatenate([first, second], axis=0)
        for direction in range(2):
            rs_copy(direction, h - 1, k).wait_recv()
            value = value + rs_recv[direction, h - 1, :, cols].astype(jnp.float32)
        xg[m, :, pl.ds(pl.multiple_of(g * half + k * sub, sub), sub)] = value.astype(jnp.bfloat16)
        copy = half_copy(m, g, 0, k)
        copy.start()
        pending.append((copy, None))
        if h > 1 or travels(0, k):
            copy = ag_copy(0, 0, k, m)
            copy.start()
            pending.append((copy, None))

    for turn in range(SUBS):
        k = (turn + SUBS // 2) % SUBS
        if h > 1 or travels(1, k):
            copy = ag_copy(1, 0, k, m)
            copy.start()
            pending.append((copy, None))

    order = [m]
    for s in range(h - 1):
        order += [chip_at(place - 1 - s), chip_at(place + 1 + s)]
    order.append(chip_at(place + h))
    stages = [(0, 1)] + [(1 + 2 * s, 2) for s in range(h - 1)] + [(n - 1, 1)]
    per_group = parts // groups
    count = n // per_group
    own_group = c // per_group

    def keeper(group, holder):
        return group * per_group + holder // count

    def slot_of(source, target):
        return 0 if parts == 2 else lax.rem(source - target + parts, parts) - 1

    def ex_copy(source, target, stage, t):
        first, size = stage
        where = (slot_of(source, target), t, slice(None), pl.ds(first, size))
        return remote(
            ex_send.at[where],
            ex_recv.at[where],
            ex_send_sem.at[slot_of(source, target), t, first],
            ex_recv_sem.at[slot_of(source, target), t, first],
            (g, m, target),
        )

    def sq_copy(source, target, stage):
        first, size = stage
        where = (slot_of(source, target), pl.ds(first, size))
        return remote(
            sq_send.at[where],
            sq_recv.at[where],
            sq_send_sem.at[slot_of(source, target), first],
            sq_recv_sem.at[slot_of(source, target), first],
            (g, m, target),
        )

    def items(stage):
        first, size = stage
        if per_group == 1:
            return [stage]
        return [(first + i, 1) for i in range(size)]

    def mine_to_keep(j, item):
        if j > 0:
            return False, None
        if per_group == 1:
            return True, None
        return None, order[item[0]] // count == lax.rem(c, per_group)

    def pack_squares(column):
        lane = lax.broadcasted_iota(jnp.int32, (8, 128), 1)
        packed = jnp.zeros((8, 128), jnp.float32)
        for a in range(rows // 8):
            packed = packed + jnp.where(lane == a, column[8 * a : 8 * a + 8], 0.0)
        return packed

    def route(j, item, keep_it, send_it):
        certain, condition = mine_to_keep(j, item)
        if certain is None:
            pl.when(condition)(keep_it)
            pl.when(jnp.logical_not(condition))(send_it)
        elif certain:
            keep_it()
        else:
            send_it()

    def run_stage(stage):
        first, size = stage
        for i in range(first, first + size):
            wide = xg[order[i]].astype(jnp.float32)
            summed = jnp.sum(wide * wide, axis=1, keepdims=True)
            squares[i] = jnp.broadcast_to(summed, (groups * rows, 128)).reshape(groups, rows, 128)
        for item in items(stage):
            for j in range(groups):
                group = lax.rem(own_group + j, groups)
                target = keeper(group, order[item[0]])

                def keep_it(item=item, group=group):
                    for i in range(item[0], item[0] + item[1]):
                        sq_keep[i] = pack_squares(squares[i, group])

                def send_it(item=item, group=group, target=target):
                    for i in range(item[0], item[0] + item[1]):
                        sq_send[slot_of(c, target), i] = pack_squares(squares[i, group])
                    sq_copy(c, target, item).start()

                route(j, item, keep_it, send_it)

        def expand(t, carry):
            cols = pl.ds(pl.multiple_of(t * tile, tile), tile)
            lhs = jnp.concatenate([xg[order[i]] for i in range(first, first + size)], axis=0)
            for w, weights in enumerate((gate_buf, up_buf)):
                value = jnp.dot(lhs, weights[:, cols], preferred_element_type=jnp.float32)
                result[w, :size] = value.reshape(size, groups, rows, tile)
            for item in items(stage):
                local = pl.ds(item[0] - first, item[1])
                for j in range(groups):
                    group = lax.rem(own_group + j, groups)
                    target = keeper(group, order[item[0]])

                    def keep_it(item=item, local=local, group=group):
                        keep[t, :, pl.ds(item[0], item[1])] = result[:, local, group]

                    def send_it(item=item, local=local, group=group, target=target):
                        ex_send[slot_of(c, target), t, :, pl.ds(item[0], item[1])] = result[
                            :, local, group
                        ].astype(jnp.bfloat16)
                        ex_copy(c, target, item, t).start()

                    route(j, item, keep_it, send_it)
            return carry

        lax.fori_loop(0, tiles, expand, 0)

    gate_load.wait()
    up_load.wait()
    res_store = pltpu.make_async_copy(res_out, res_out_hbm, load_sem.at[5])
    for s in range(-1, h):
        for turn in range(SUBS):
            if s < 0:
                break
            for direction in range(2):
                k = turn if direction == 0 else (turn + SUBS // 2) % SUBS
                last = s == h - 1
                if last and not travels(direction, k):
                    continue
                holder = chip_at(place - 1 - s if direction == 0 else place + 1 + s)
                slot = n - 1 if last else 1 + 2 * s + direction
                ag_copy(direction, s, k, holder).wait_recv()
                if s + 1 < h and (s + 1 < h - 1 or travels(direction, k)):
                    copy = ag_copy(direction, s + 1, k, holder)
                    copy.start()
                    pending.append((copy, None))
                copy = half_copy(holder, g, slot, k)
                copy.start()
                pending.append((copy, None))
        stage = stages[s + 1]
        for i in range(stage[0], stage[0] + stage[1]):
            for k in range(SUBS):
                half_copy(order[i], 1 - g, i, k).wait_recv()
        if s < 0:
            both = xg[m].astype(jnp.float32)
            res_out[...] = jnp.where(g == 0, both[:rows], both[rows:]).astype(jnp.bfloat16)
            res_store.start()
        run_stage(stage)

    def finish(item):
        total = [sq_keep[i] for i in range(item[0], item[0] + item[1])]
        for k in range(1, parts):
            source = lax.rem(c + k, parts)
            sq_copy(source, c, item).wait_recv()
            total = [
                value + sq_recv[slot_of(source, c), item[0] + i] for i, value in enumerate(total)
            ]
        inverse = []
        for value in total:
            packed = lax.rsqrt(value / D + norm_epsilon)
            inverse.append(
                jnp.concatenate([packed[:, a : a + 1] for a in range(rows // 8)], axis=0)
            )

        def activate(t, carry):
            for k in range(1, parts):
                ex_copy(lax.rem(c + k, parts), c, item, t).wait_recv()
            cols = pl.ds(pl.multiple_of(t * tile, tile), tile)
            for i, scale in enumerate(inverse):
                sums = []
                for w in range(2):
                    value = keep[t, w, item[0] + i]
                    for k in range(1, parts):
                        slot = slot_of(lax.rem(c + k, parts), c)
                        value = value + ex_recv[slot, t, w, item[0] + i].astype(jnp.float32)
                    sums.append(value * scale)
                gate, up = sums
                holder = order[item[0] + i]
                act_out[lax.rem(holder, count), :, cols] = (
                    gate / (1.0 + jnp.exp(-gate)) * up
                ).astype(jnp.bfloat16)
            return carry

        lax.fori_loop(0, tiles, activate, 0)
        for i in range(item[0], item[0] + item[1]):
            store(lax.rem(order[i], count)).start()

    def store(index):
        return pltpu.make_async_copy(
            act_out.at[index], act_out_hbm.at[index], store_sem.at[index]
        )

    def sent(item, target):
        sq_copy(c, target, item).wait_send()

        def each(t, carry):
            ex_copy(c, target, item, t).wait_send()
            return carry

        lax.fori_loop(0, tiles, each, 0)

    for stage in stages:
        for item in items(stage):
            route(0, item, functools.partial(finish, item), lambda: None)
            for j in range(groups):
                target = keeper(lax.rem(own_group + j, groups), order[item[0]])
                route(j, item, lambda: None, functools.partial(sent, item, target))

    res_store.wait()
    for i in range(count):
        store(i).wait()
    for copy, condition in pending:
        if condition is None:
            copy.wait_send()
        else:
            pl.when(condition)(copy.wait_send)


def layer(sizes, attended, residual_in, out_weight, gate_weight, up_weight):
    groups, n, parts = sizes
    h = n // 2
    rows, width = attended.shape
    feat = out_weight.shape[0]
    half = width // 2
    hidden = gate_weight.shape[1]
    tile = hidden // 2 if hidden % 256 == 0 else 128
    tiles = hidden // tile
    kept = groups * n * rows // parts
    bf16, f32 = jnp.bfloat16, jnp.float32
    dma = pltpu.SemaphoreType.DMA
    hbm = pl.BlockSpec(memory_space=pltpu.HBM)
    blocks = width // feat
    residual_out, activation = pl.pallas_call(
        functools.partial(layer_kernel, sizes),
        out_shape=(
            jax.ShapeDtypeStruct((rows, width), bf16),
            jax.ShapeDtypeStruct((kept // rows, rows, hidden), bf16),
        ),
        in_specs=[hbm] * 5,
        out_specs=(hbm, hbm),
        scratch_shapes=[
            pltpu.VMEM((rows, width), bf16),
            pltpu.VMEM((rows, width), bf16),
            pltpu.VMEM((rows, width), bf16),
            pltpu.VMEM((kept // rows, rows, hidden), bf16),
            pltpu.VMEM((groups, feat, half), bf16),
            pltpu.VMEM(gate_weight.shape, bf16),
            pltpu.VMEM(up_weight.shape, bf16),
            pltpu.VMEM((rows, half), bf16),
            pltpu.VMEM((groups, groups * n, rows, feat), bf16),
            pltpu.VMEM((n, groups * rows, groups * feat), bf16),
            pltpu.VMEM((n, groups * rows, half), f32),
            pltpu.VMEM((2, h, groups * rows, half), bf16),
            pltpu.VMEM((2, h, groups * rows, half), bf16),
            pltpu.VMEM((n, groups * rows, width), bf16),
            pltpu.VMEM((n, groups, rows, 128), f32),
            pltpu.VMEM((n, 8, 128), f32),
            pltpu.VMEM((parts - 1, n, 8, 128), f32),
            pltpu.VMEM((parts - 1, n, 8, 128), f32),
            pltpu.VMEM((2, 2, groups, rows, tile), f32),
            pltpu.VMEM((tiles, 2, n, rows, tile), f32),
            pltpu.VMEM((parts - 1, tiles, 2, n, rows, tile), bf16),
            pltpu.VMEM((parts - 1, tiles, 2, n, rows, tile), bf16),
            dma((6,)),
            dma((kept // rows,)),
            dma((2,)),
            dma((2,)),
            dma((parts, blocks)),
            dma((groups * n,)),
            dma((groups * n,)),
            dma((groups * n,)),
            dma((2, h, SUBS)),
            dma((2, h, SUBS)),
            dma((2, h, SUBS)),
            dma((2, h, SUBS)),
            dma((n, SUBS)),
            dma((n, SUBS)),
            dma((parts - 1, n)),
            dma((parts - 1, n)),
            dma((parts - 1, tiles, n)),
            dma((parts - 1, tiles, n)),
        ],
        compiler_params=pltpu.CompilerParams(
            collective_id=0, has_side_effects=True, vmem_limit_bytes=56 * 1024 * 1024
        ),
    )(attended, residual_in, out_weight, gate_weight, up_weight)
    residual_out, activation = hand_over(residual_out, activation)
    return residual_out, activation.reshape(kept, hidden)


def hand_over_kernel(res_in, act_in, res_out, act_out, res_buf, act_buf, in_sem, out_sem):
    chips = act_in.shape[0]
    moves = [
        (
            pltpu.make_async_copy(res_in, res_buf, in_sem.at[chips]),
            pltpu.make_async_copy(res_buf, res_out, out_sem.at[chips]),
        )
    ]
    for i in range(chips):
        moves.append(
            (
                pltpu.make_async_copy(act_in.at[i], act_buf.at[i], in_sem.at[i]),
                pltpu.make_async_copy(act_buf.at[i], act_out.at[i], out_sem.at[i]),
            )
        )
    for into, _ in moves:
        into.start()
    for into, out in moves:
        into.wait()
        out.start()
    for _, out in moves:
        out.wait()


def hand_over(residual_out, activation):
    hbm = pl.BlockSpec(memory_space=pltpu.HBM)
    dma = pltpu.SemaphoreType.DMA((activation.shape[0] + 1,))
    return pl.pallas_call(
        hand_over_kernel,
        out_shape=tuple(
            jax.ShapeDtypeStruct(x.shape, x.dtype) for x in (residual_out, activation)
        ),
        in_specs=[hbm, hbm],
        out_specs=(hbm, hbm),
        scratch_shapes=[
            pltpu.VMEM(residual_out.shape, residual_out.dtype),
            pltpu.VMEM(activation.shape, activation.dtype),
            dma,
            dma,
        ],
        compiler_params=pltpu.CompilerParams(vmem_limit_bytes=56 * 1024 * 1024),
    )(residual_out, activation)


def body(
    queries,
    new_keys,
    new_values,
    key_cache,
    value_cache,
    context_len,
    cache_slot,
    residual_in,
    out_weight,
    gate_weight,
    up_weight,
):
    attended = attend_rows(
        queries, new_keys, new_values, key_cache, value_cache, context_len, cache_slot
    )
    sizes = (lax.axis_size("grp"), lax.axis_size("mr"), lax.axis_size("mc"))
    return layer(sizes, attended, residual_in, out_weight, gate_weight, up_weight)


def solution(mesh):
    in_specs = (
        P(("grp", "mr"), "mc"),
        P(("grp", "mr"), "mc"),
        P(("grp", "mr"), "mc"),
        P(("grp", "mr"), None, "mc"),
        P(("grp", "mr"), None, "mc"),
        P(("grp", "mr")),
        P(("grp", "mr")),
        P(("grp", "mr"), "mc"),
        P(("grp", "mr"), "mc"),
        P("mc", ("grp", "mr")),
        P("mc", ("grp", "mr")),
    )
    out_specs = (P(("grp", "mr"), "mc"), P("mc", ("grp", "mr")))
    return jax.shard_map(body, mesh=mesh, in_specs=in_specs, out_specs=out_specs, check_vma=False)
```
